32 devices in a mesh: section: 2 (over core), expert: 16 (over z, y, x).
Axes of the slice: x: 2, y: 2, z: 4, core: 2. Of those that a mesh axis runs over, the one named last changes fastest.
Arguments:
- tokens: bfloat16 [2, 1024, 2048], P(None, 'expert'), may hold values from -6 to 6
- norm_gain: float32 [2, 2048], P('section'), may hold values from 0.5 to 2
- gate_weight: bfloat16 [2, 16, 2048, 768], P('section', 'expert'), may hold values from -0.125 to 0.125
- up_weight: bfloat16 [2, 16, 2048, 768], P('section', 'expert'), may hold values from -0.125 to 0.125
- down_weight: bfloat16 [2, 16, 768, 2048], P('section', 'expert'), may hold values from -0.21875 to 0.21875
- expert_place: int32 [2, 16], P('section'), may hold values from 0 to 15, each once within a row
- expert_ids: int32 [2, 2, 1024, 8], P('section', None, 'expert'), may hold values from 0 to 15, all different within a row; in each aligned block of 64 rows (0 to 63, 64 to 127, ..., all dimensions but the last counted through in order) at most 40 rows name the same one
- route_weights: float32 [2, 2, 1024, 8], P('section', None, 'expert'), may hold values from 0.05 to 0.4
Outputs:
- final_states: bfloat16 [2, 1024, 2048], P(None, 'expert')
The draws below stay inside these ranges and needn't reach their ends.
Inputs may be any that keep to these rules, and one draw needn't show every extreme that they name: `expert_ids`: each row names 8 different experts. In each aligned block of 64 rows (one device's tokens of one micro-batch in one layer) no expert is named by more than 40 rows, a bound that some block reaches. `expert_place`: each layer's row names every index along expert once.
All inputs are finite; a program needn't handle non-finite values.
Results may differ from the reference program's by a relative error of at most 0.013.
Values may be sent and summed in bfloat16 or wider, within the bound.
A program may use at most 128 MiB of HBM per device.

```python
import math
import jax
import jax.numpy as jnp
import numpy as np
from jax import lax

D = 2048
FFE = 768
TOPK = 8
MB = 2
TOK_DEV = 64
EXPERTS = 16
LAYERS = 2
TOKENS = 1024
CAP = 40
N_EXPERT = 16


def level_of(stream_key, dims, split, smallest, top_value):
    factor_of = 1.0
    for axis_at, parts in split:
        draws = jax.random.uniform(jax.random.fold_in(jax.random.fold_in(stream_key, 6), axis_at), (parts,), jnp.float32, smallest / len(split), top_value / len(split))
        factor_of = factor_of * jnp.repeat(jnp.exp(draws), dims[axis_at] // parts).reshape((-1,) + (1,) * (len(dims) - 1 - axis_at))
    return factor_of


def deal_out(own_key, own, number, rows, number_of, top, reach, lean):
    order = jax.random.permutation(own_key, number_of)
    crowded, common = portions_of(number_of, rows * top, reach, lean, True), portions_of(number_of, rows * top, reach, lean, False)
    places = jnp.arange(number_of)

    def named(lengths, rotation):
        used = int((lengths > 0).sum())
        fixed = max(1, used // 4)
        moved = fixed + (places - fixed + rotation * (used - fixed)) % max(1, number_of - fixed)
        return jnp.zeros((number_of,), jnp.int32).at[order[jnp.where(places < fixed, places, moved)]].set(jnp.asarray(lengths, jnp.int32))

    lengths = jnp.where(number % 4 == 0, named(crowded, number // 4), named(common, number - number // 4 - 1))
    mixed = jax.random.permutation(jax.random.fold_in(own, 3), number_of)
    source_of, sink = mixed[0:number_of // 2 * 2:2], mixed[1:number_of // 2 * 2:2]
    room = jnp.minimum(lengths[source_of] - 1, reach - lengths[sink]) // 2
    room = jnp.where((source_of == order[0]) | (sink == order[0]) | (lengths[sink] == 0), 0, jnp.maximum(room, 0))
    moved = jax.random.randint(jax.random.fold_in(own, 4), (number_of // 2,), 0, 1 << 20) % (room + 1)
    lengths = lengths.at[source_of].add(-moved).at[sink].add(moved)
    items = jnp.searchsorted(jnp.cumsum(lengths), jnp.arange(rows * top), side="right").astype(jnp.int32)
    table = items.reshape(top, rows).T
    table = table[jax.random.permutation(jax.random.fold_in(own, 1), rows)]
    rotation = jax.random.randint(jax.random.fold_in(own, 2), (rows, 1), 0, top)
    return jnp.take_along_axis(table, (jnp.arange(top)[None, :] + rotation) % top, axis=1)


def portions_of(number_of, total, limit, skew, full):
    weights = [(1 << 20) // math.isqrt(grade ** skew) + 1 for grade in range(1, number_of + 1)]
    largest = limit if full else min(limit, max(-(-total // number_of), total * weights[0] // sum(weights)))
    least = 1 if total - largest >= number_of - 1 else 0
    counts, spare = [largest] + [least] * (number_of - 1), total - largest - least * (number_of - 1)
    while spare > 0:
        candidates = [i for i in range(1, number_of) if counts[i] < largest] or [i for i in range(1, number_of) if counts[i] < limit]
        pool, left = sum([weights[i] for i in candidates]), spare
        for i in candidates:
            more = min(limit - counts[i], max(1, left * weights[i] // pool), spare)
            counts[i] = counts[i] + more
            spare = spare - more
    return np.array(counts)


def bell_draw(rng, extent, deviation, most, cuts=(), held_as=jnp.bfloat16):
    entries = deviation * jax.random.normal(rng, extent, jnp.float32)
    if cuts:
        entries = entries * level_of(rng, extent, cuts, -0.22, 0.18)
    return jnp.clip(entries, -most, most).astype(held_as)


def setup_inputs(seed: int = 0) -> dict:
    splits = jax.random.split(jax.random.key(seed), 9)
    tokens = bell_draw(splits[0], (MB, TOKENS, D), 1.0, 6.0, ((1, 16),))
    norm_gain = jnp.clip(jnp.exp(math.log(2.0) - 1.3862944 * jax.random.uniform(splits[1], (LAYERS, D), jnp.float32) ** level_of(splits[1], (LAYERS, D), ((0, 2),), -0.2, 0.2)), 0.5, 2.0)
    gate_weight = bell_draw(splits[2], (LAYERS, EXPERTS, D, FFE), D ** -0.5, 0.125, ((0, 2), (1, 16)))
    up_weight = bell_draw(splits[3], (LAYERS, EXPERTS, D, FFE), D ** -0.5, 0.125, ((0, 2), (1, 16)))
    down_weight = bell_draw(splits[4], (LAYERS, EXPERTS, FFE, D), FFE ** -0.5, 0.21875, ((0, 2), (1, 16)))
    expert_place = jax.vmap(lambda own: jax.random.permutation(own, EXPERTS))(jax.random.split(splits[5], LAYERS)).reshape((LAYERS, EXPERTS)).astype(jnp.int32)
    expert_ids_keys = jax.random.split(jax.random.fold_in(splits[6], 1), LAYERS * MB * TOKENS // TOK_DEV)
    expert_ids_turns = jax.random.permutation(jax.random.fold_in(splits[6], 3), LAYERS * MB * TOKENS // TOK_DEV)
    expert_ids = jax.vmap(lambda own, number: deal_out(jax.random.fold_in(splits[6], 2), own, number, TOK_DEV, EXPERTS, TOPK, CAP, 2))(expert_ids_keys, expert_ids_turns).reshape((LAYERS, MB, TOKENS, TOPK))
    route_weights = jnp.clip(0.05 + 0.35 * jax.random.uniform(splits[7], (LAYERS, MB, TOKENS, TOPK), jnp.float32) ** level_of(splits[7], (LAYERS, MB, TOKENS, TOPK), ((0, 2), (2, 16)), -0.2, 0.2), 0.05, 0.4)
    return dict(tokens=tokens, norm_gain=norm_gain, gate_weight=gate_weight, up_weight=up_weight, down_weight=down_weight, expert_place=expert_place, expert_ids=expert_ids, route_weights=route_weights)


EPSILON = 1e-06

def normalize(values, gain_row):
    widened = values.astype(jnp.float32)
    inverse_rms = lax.rsqrt(lax.optimization_barrier(jnp.mean(widened * widened, axis=-1, keepdims=True)) + EPSILON)
    return (widened * inverse_rms * gain_row[None, :]).astype(jnp.bfloat16)

def slot_positions(block_ids):
    onehot = (block_ids[..., None] == jnp.arange(EXPERTS, dtype=jnp.int32)).astype(jnp.int32)
    before = jnp.cumsum(onehot, axis=1) - onehot
    return lax.optimization_barrier(jnp.sum(before * onehot, axis=-1)).astype(jnp.int32)

def moe_layer(hidden, gain_row, gate_matrix, up_matrix, down_matrix, holder_table, chosen, weights):
    normed = normalize(hidden, gain_row)
    block_ids = chosen.reshape(N_EXPERT, TOK_DEV * TOPK)
    position = slot_positions(block_ids).reshape(-1)
    flat_ids = chosen.reshape(-1).astype(jnp.int32)
    entry_index = jnp.arange(TOKENS * TOPK, dtype=jnp.int32)
    source = entry_index // (TOK_DEV * TOPK)
    target = (flat_ids * N_EXPERT + source) * CAP + position
    token_row = entry_index // TOPK
    buffer = jnp.zeros((EXPERTS * N_EXPERT * CAP, D), jnp.bfloat16).at[target].set(normed[token_row])
    buffer = buffer.reshape(EXPERTS, N_EXPERT * CAP, D)

    def run_expert(expert):
        holder = holder_table[expert]
        row_block = buffer[expert]
        gate_part = jnp.dot(row_block, gate_matrix[holder], preferred_element_type=jnp.float32)
        up_part = jnp.dot(row_block, up_matrix[holder], preferred_element_type=jnp.float32)
        hidden_units = (jax.nn.silu(gate_part) * up_part).astype(jnp.bfloat16)
        return jnp.dot(hidden_units, down_matrix[holder], preferred_element_type=jnp.float32).astype(jnp.bfloat16)
    outputs = lax.map(run_expert, jnp.arange(EXPERTS, dtype=jnp.int32)).reshape(-1, D)
    picked = outputs[target].astype(jnp.float32).reshape(TOKENS, TOPK, D)
    mixture = jnp.einsum('tk,tkd->td', weights.astype(jnp.float32), picked)
    return (hidden.astype(jnp.float32) + mixture).astype(jnp.bfloat16)

def reference(tokens, norm_gain, gate_weight, up_weight, down_weight, expert_place, expert_ids, route_weights):
    finals = []
    for micro_index in range(MB):
        hidden = tokens[micro_index]
        for layer_index in range(LAYERS):
            hidden = moe_layer(hidden, norm_gain[layer_index], gate_weight[layer_index], up_weight[layer_index], down_weight[layer_index], expert_place[layer_index], expert_ids[layer_index, micro_index], route_weights[layer_index, micro_index])
        finals.append(hidden)
    return jnp.stack(finals)
```

```python
import functools

import jax
import jax.numpy as jnp
from jax import lax
from jax.experimental import pallas as pl
from jax.experimental.pallas import tpu as pltpu
from jax.sharding import PartitionSpec as P

EPSILON = 1e-06


def from_behind(array, axis, by):
    size = lax.axis_size(axis)
    return lax.ppermute(array, axis, [(i, (i + by) % size) for i in range(size)])


def normalize(values, gain_row):
    widened = values.astype(jnp.float32)
    inverse_rms = lax.rsqrt(jnp.mean(widened * widened, axis=-1, keepdims=True) + EPSILON)
    return (widened * inverse_rms * gain_row[None, :]).astype(jnp.bfloat16)


def expert_ffn(row_block, gate_matrix, up_matrix, down_matrix):
    gate_part = jnp.dot(row_block, gate_matrix, preferred_element_type=jnp.float32)
    up_part = jnp.dot(row_block, up_matrix, preferred_element_type=jnp.float32)
    hidden_units = (jax.nn.silu(gate_part) * up_part).astype(jnp.bfloat16)
    return jnp.dot(hidden_units, down_matrix, preferred_element_type=jnp.float32).astype(
        jnp.bfloat16
    )


def routed_local(
    tokens, norm_gain, gate_weight, up_weight, down_weight, expert_place, expert_ids, route_weights
):
    sections = lax.axis_size("section")
    groups = lax.axis_size("expert")
    section_index = lax.axis_index("section")
    micro_count = tokens.shape[0]
    tok_rows = tokens.shape[1]
    model_width = tokens.shape[2]
    top_count = expert_ids.shape[3]
    experts_all = expert_place.shape[1]
    capacity = max(2, 5 * tok_rows * top_count // (4 * experts_all))
    expert_lanes = jnp.arange(experts_all, dtype=jnp.int32)
    flat_token = jnp.arange(tok_rows * top_count, dtype=jnp.int32) // top_count
    own_params = (
        norm_gain[0],
        gate_weight[0, 0],
        up_weight[0, 0],
        down_weight[0, 0],
        expert_place[0],
        expert_ids[0],
        route_weights[0],
    )

    def run_rows(received, active, params):
        row_shape = received.shape
        flat_rows = received.reshape(-1, model_width)
        computed = lax.cond(
            active,
            lambda row_block: expert_ffn(row_block, params[1], params[2], params[3]),
            lambda row_block: jnp.zeros_like(row_block),
            flat_rows,
        )
        return computed.reshape(row_shape)

    def layer_step(hidden, micro_index, active, params):
        normed = normalize(hidden, params[0])
        holder_table = params[4]
        chosen = lax.dynamic_index_in_dim(params[5], micro_index, 0, keepdims=False).reshape(-1)
        weights = lax.dynamic_index_in_dim(params[6], micro_index, 0, keepdims=False)
        onehot = (chosen[:, None] == expert_lanes[None, :]).astype(jnp.int32)
        before = jnp.cumsum(onehot, axis=0) - onehot
        position = jnp.sum(before * onehot, axis=1)
        holder = jnp.sum(onehot * holder_table[None, :], axis=1)
        target = holder * capacity + position
        outgoing = (
            jnp.zeros((groups * capacity, model_width), jnp.bfloat16)
            .at[target]
            .set(normed[flat_token])
        )
        outgoing = outgoing.reshape(groups, capacity, model_width)
        received = lax.all_to_all(outgoing, "expert", split_axis=0, concat_axis=0, tiled=True)
        returned_rows = lax.all_to_all(
            run_rows(received, active, params), "expert", split_axis=0, concat_axis=0, tiled=True
        )
        picked = returned_rows.reshape(groups * capacity, model_width)[target]
        picked = picked.astype(jnp.float32).reshape(tok_rows, top_count, model_width)
        mixture = jnp.einsum("tk,tkd->td", weights, picked)
        return (hidden.astype(jnp.float32) + mixture).astype(jnp.bfloat16)

    other_mats = from_behind((own_params[1], own_params[2], own_params[3]), "section", 1)
    other_ints = from_behind((own_params[4], own_params[5]), "section", 1)
    other_floats = from_behind((own_params[0], own_params[6]), "section", 1)
    other_params = (
        other_floats[0],
        other_mats[0],
        other_mats[1],
        other_mats[2],
        other_ints[0],
        other_ints[1],
        other_floats[1],
    )
    is_first = section_index == 0
    first_params = tuple(
        (jnp.where(is_first, mine, theirs) for mine, theirs in zip(own_params, other_params))
    )
    second_params = tuple(
        (jnp.where(is_first, theirs, mine) for mine, theirs in zip(own_params, other_params))
    )
    share = micro_count // sections
    always = jnp.array(True)
    micro_index = section_index * share + 0
    hidden = lax.dynamic_index_in_dim(tokens, micro_index, 0, keepdims=False)
    hidden = layer_step(hidden, micro_index, always, first_params)
    hidden = layer_step(hidden, micro_index, always, second_params)
    own_finals = [hidden]
    return lax.all_gather(jnp.stack(own_finals), "section", axis=0, tiled=True)


def layer_kernel(
    layer,
    depth,
    normed_ref,
    hidden_ref,
    share_ref,
    gate_hbm,
    up_hbm,
    down_hbm,
    out_ref,
    gate_mat,
    up_mat,
    down_mat,
    held,
    parts,
    from_x_half,
    from_y_half,
    from_x,
    from_y,
    from_z,
    sends,
    arrivals,
    mat_sends,
    mat_arrivals,
):
    section = lax.axis_index("section")
    me = lax.axis_index("expert")
    level = me // 4
    plane = lax.rem(me, 4)
    beside_x = level * 4 + plane + 1 - 2 * lax.rem(plane, 2)
    beside_y = level * 4 + lax.rem(plane + 2, 4)
    rows = normed_ref.shape[0]
    half = rows // 2

    def at_level(offset):
        return lax.rem(level + offset + depth, depth) * 4 + plane

    barrier = pltpu.get_barrier_semaphore()
    partners = [{"expert": beside_x}, {"expert": beside_y}, {"section": 1 - section}]
    partners += [{"expert": at_level(k)} for k in range(1, depth)]
    for partner in partners:
        pl.semaphore_signal(
            barrier, inc=1, device_id=partner, device_id_type=pl.DeviceIdType.MESH
        )
    pl.semaphore_wait(barrier, len(partners))

    started = []

    def send(kind, k, source, target, peer):
        copy = pltpu.make_async_remote_copy(
            src_ref=source,
            dst_ref=target,
            send_sem=sends.at[kind, k],
            recv_sem=arrivals.at[kind, k],
            device_id={"expert": peer},
            device_id_type=pl.DeviceIdType.MESH,
        )
        copy.start()
        started.append(copy)
        return copy

    lower, upper = pl.ds(0, half), pl.ds(half, rows - half)

    by_z = [None] + [
        send(0, k, normed_ref, held.at[k, 0], at_level(k)) for k in range(1, depth)
    ]
    by_x = {0: send(1, 0, normed_ref, held.at[0, 1], beside_x)}
    by_y = {0: send(2, 0, normed_ref, held.at[0, 2], beside_y)}

    mats = [(gate_hbm, gate_mat), (up_hbm, up_mat), (down_hbm, down_mat)]
    remote_mats = [
        pltpu.make_async_remote_copy(
            src_ref=source,
            dst_ref=target,
            send_sem=mat_sends.at[i],
            recv_sem=mat_arrivals.at[i],
            device_id={"section": 1 - section},
            device_id_type=pl.DeviceIdType.MESH,
        )
        for i, (source, target) in enumerate(mats)
    ]
    local_mats = [
        pltpu.make_async_copy(source, target, mat_sends.at[3 + i])
        for i, (source, target) in enumerate(mats)
    ]

    @pl.when(section == layer)
    def _():
        for copy in remote_mats + local_mats:
            copy.start()

    held[0, 0] = normed_ref[...]

    by_xy, by_yx = {}, {}

    def relay(k):
        by_z[k].wait_recv()
        by_x[k] = send(1, k, held.at[k, 0], held.at[k, 1], beside_x)
        by_y[k] = send(2, k, held.at[k, 0], held.at[k, 2], beside_y)

    def relay_diagonal(k):
        by_x[k].wait_recv()
        by_xy[k] = send(3, k, held.at[k, 1, lower], held.at[k, 3, lower], beside_y)
        by_y[k].wait_recv()
        by_yx[k] = send(4, k, held.at[k, 2, upper], held.at[k, 3, upper], beside_x)

    halves_y, halves_x, fulls_x, fulls_y, backs = {}, {}, {}, {}, {}

    def compute(k):
        by_xy[k].wait_recv()
        by_yx[k].wait_recv()
        block = held[k].reshape(4 * rows, held.shape[3])
        gate_part = jnp.dot(block, gate_mat[...], preferred_element_type=jnp.float32)
        up_part = jnp.dot(block, up_mat[...], preferred_element_type=jnp.float32)
        hidden_units = (gate_part / (1.0 + jnp.exp(-gate_part)) * up_part).astype(jnp.bfloat16)
        out = jnp.dot(hidden_units, down_mat[...], preferred_element_type=jnp.float32)
        out = out.astype(jnp.bfloat16).astype(jnp.float32) * share_ref[k]
        parts[k] = out.astype(jnp.bfloat16).reshape(parts.shape[1:])
        halves_y[k] = send(5, k, parts.at[k, 3, lower], from_y_half.at[k], beside_y)
        halves_x[k] = send(6, k, parts.at[k, 3, upper], from_x_half.at[k], beside_x)

    def add(*terms):
        total = terms[0].astype(jnp.float32)
        for term in terms[1:]:
            total = total + term.astype(jnp.float32)
        return total

    def combine_half(k):
        halves_y[k].wait_recv()
        parts[k, 1, lower] = add(parts[k, 1, lower], from_y_half[k]).astype(jnp.bfloat16)
        fulls_x[k] = send(7, k, parts.at[k, 1], from_x.at[k], beside_x)
        halves_x[k].wait_recv()
        parts[k, 2, upper] = add(parts[k, 2, upper], from_x_half[k]).astype(jnp.bfloat16)
        fulls_y[k] = send(8, k, parts.at[k, 2], from_y.at[k], beside_y)

    def combine_full(k):
        fulls_x[k].wait_recv()
        fulls_y[k].wait_recv()
        parts[k, 0] = add(parts[k, 0], from_x[k], from_y[k]).astype(jnp.bfloat16)
        backs[k] = send(9, k, parts.at[k, 0], from_z.at[k], at_level(-k))

    def wait_mats():
        @pl.when(section == layer)
        def _():
            for copy in remote_mats:
                copy.wait_send()
            for copy in local_mats:
                copy.wait()

        @pl.when(section != layer)
        def _():
            for copy in remote_mats:
                copy.wait_recv()

    relay(1)
    relay_diagonal(0)
    for k in range(depth):
        if k + 2 < depth:
            relay(k + 2)
        if k + 1 < depth:
            relay_diagonal(k + 1)
        if k == 0:
            wait_mats()
        compute(k)
        if k >= 1:
            combine_half(k - 1)
        if k >= 2:
            if k > 2:
                combine_full(k - 2)
    combine_half(depth - 1)
    for k in range(max(1, depth - 2), depth):
        combine_full(k)
    fulls_x[0].wait_recv()
    fulls_y[0].wait_recv()
    mixture = add(parts[0, 0], from_x[0], from_y[0])
    for k in range(1, depth):
        backs[k].wait_recv()
        mixture = mixture + from_z[k].astype(jnp.float32)
    out_ref[...] = (hidden_ref[...].astype(jnp.float32) + mixture).astype(jnp.bfloat16)
    for copy in started:
        copy.wait_send()


def layer_call(layer, depth, normed, hidden, share, gate_matrix, up_matrix, down_matrix):
    rows, width = normed.shape
    vmem = pl.BlockSpec(memory_space=pltpu.VMEM)
    anywhere = pl.BlockSpec(memory_space=pl.ANY)
    bf16 = jnp.bfloat16
    return pl.pallas_call(
        functools.partial(layer_kernel, layer, depth),
        out_shape=jax.ShapeDtypeStruct((rows, width), bf16),
        in_specs=[vmem, vmem, vmem, anywhere, anywhere, anywhere],
        out_specs=vmem,
        scratch_shapes=[
            pltpu.VMEM(gate_matrix.shape, bf16),
            pltpu.VMEM(up_matrix.shape, bf16),
            pltpu.VMEM(down_matrix.shape, bf16),
            pltpu.VMEM((depth, 4, rows, width), bf16),
            pltpu.VMEM((depth, 4, rows, width), bf16),
            pltpu.VMEM((depth, rows // 2, width), bf16),
            pltpu.VMEM((depth, rows // 2, width), bf16),
            pltpu.VMEM((depth, rows, width), bf16),
            pltpu.VMEM((depth, rows, width), bf16),
            pltpu.VMEM((depth, rows, width), bf16),
            pltpu.SemaphoreType.DMA((10, depth)),
            pltpu.SemaphoreType.DMA((10, depth)),
            pltpu.SemaphoreType.DMA((6,)),
            pltpu.SemaphoreType.DMA((3,)),
        ],
        compiler_params=pltpu.CompilerParams(
            collective_id=layer,
            has_side_effects=True,
            vmem_limit_bytes=56 * 1024 * 1024,
        ),
    )(normed, hidden, share, gate_matrix, up_matrix, down_matrix)


def dense_local(
    tokens, norm_gain, gate_weight, up_weight, down_weight, expert_place, expert_ids, route_weights
):
    groups = lax.axis_size("expert")
    section_index = lax.axis_index("section")
    expert_index = lax.axis_index("expert")
    is_first = section_index == 0
    lanes = jnp.arange(groups, dtype=jnp.int32)
    held_by = jnp.sum(
        jnp.where(expert_ids[0][..., None] == lanes, expert_place[0], 0), axis=-1
    )
    dense = jnp.sum(
        jnp.where(held_by[..., None] == lanes, route_weights[0][..., None], 0.0), axis=2
    )
    kept = jnp.where(is_first, dense[0], dense[1])
    sent = jnp.where(is_first, dense[1], dense[0])
    swapped = from_behind(sent, "section", 1)
    both = jnp.stack([jnp.where(is_first, kept, swapped), jnp.where(is_first, swapped, kept)])
    shares = lax.all_gather(both, "expert", axis=1, tiled=True)
    shares = lax.dynamic_index_in_dim(shares, expert_index, 2, keepdims=True)

    other_gain = from_behind(norm_gain[0], "section", 1)
    gains = (
        jnp.where(is_first, norm_gain[0], other_gain),
        jnp.where(is_first, other_gain, norm_gain[0]),
    )
    depth = groups // 4
    plane = lax.rem(expert_index, 4)
    steps = jnp.arange(depth, dtype=jnp.int32)[:, None]
    columns = jnp.bitwise_xor(plane, jnp.arange(4, dtype=jnp.int32))[None, :]
    origin = (lax.rem(expert_index // 4 - steps + depth, depth) * 4 + columns).reshape(-1)
    rows = tokens.shape[1]
    shares = shares.reshape(2, groups, rows)[:, origin].reshape(2, depth, 4 * rows, 1)

    hidden = lax.dynamic_index_in_dim(tokens, section_index, 0, keepdims=False)
    for layer in range(2):
        normed = normalize(hidden, gains[layer])
        hidden = layer_call(
            layer,
            depth,
            normed,
            hidden,
            shares[layer],
            gate_weight[0, 0],
            up_weight[0, 0],
            down_weight[0, 0],
        )
    return lax.all_gather(hidden[None], "section", axis=0, tiled=True)


def local(
    tokens, norm_gain, gate_weight, up_weight, down_weight, expert_place, expert_ids, route_weights
):
    dense = 2 * expert_ids.shape[3] >= expert_place.shape[1] and tokens.shape[0] == 2
    dense = dense and lax.axis_size("expert") % 4 == 0 and lax.axis_size("expert") > 4
    run = dense_local if dense else routed_local
    return run(
        tokens,
        norm_gain,
        gate_weight,
        up_weight,
        down_weight,
        expert_place,
        expert_ids,
        route_weights,
    )


def solution(mesh):
    in_specs = (
        P(None, "expert", None),
        P("section", None),
        P("section", "expert", None, None),
        P("section", "expert", None, None),
        P("section", "expert", None, None),
        P("section", None),
        P("section", None, "expert", None),
        P("section", None, "expert", None),
    )
    out_specs = P(None, "expert", None)
    return jax.shard_map(local, mesh=mesh, in_specs=in_specs, out_specs=out_specs, check_vma=False)
```
